256 devices in a mesh: graph: 16 (over z, y_lo), row: 16 (over y_hi, x, core).
Axes of the slice: x: 4, y: 4 (y_hi: 2, y_lo: 2; y = y_hi * 2 + y_lo), z: 8, core: 2. Of those that a mesh axis runs over, the one named last changes fastest.
Arguments:
- tiles: bfloat16 [16384, 256, 256], P(('graph', 'row')), parts along dimension 0, may hold values from -0.25 to 0.25
- tile_rows: int32 [16384], P(('graph', 'row')), parts along dimension 0, may hold values from 0 to 15
- tile_cols: int32 [16384], P(('graph', 'row')), parts along dimension 0, may hold values from 0 to 255, as said below
- tile_count: int32 [256], P(('graph', 'row')), parts along dimension 0, may hold values from 8 to 64, as said below
- seeds: float32 [32, 1048576], P(None, ('graph', 'row')), parts along dimension 1, may hold values from -6 to 6
- decay: float32 [32], replicated, may hold values from 0.8 to 1
Outputs:
- scores: float32 [32, 1048576], P(None, ('graph', 'row')), parts along dimension 1
The draws below stay inside these ranges and needn't reach their ends.
There are 16 independent parts, one for each index of `graph`. The reference program is written for one: setup_inputs(seed, part) draws one part's arguments, and reference() takes and returns one part's arrays. A program takes and returns all parts, laid end to end along the dimension named above; an argument that names none is the same for every part. Nothing has to cross between parts.
Inputs may be any that keep to these rules, and one draw needn't show every extreme that they name: `tile_cols`: among the slots of one row panel, the tile columns that fall in the 16 tile rows of any one panel take at most 4 distinct values; in every draw the live slots of some panel take exactly 4 distinct tile columns of some one panel. Only the first tile_count slots of a panel are live; in every draw one panel has all 64 slots live.
All inputs are finite; a program needn't handle non-finite values.
Results may differ from the reference program's by a relative error of at most 0.0027.
Values may be sent and summed in bfloat16 or wider, within the bound.
No kernel may reach another device: no remote copies, remote signals or barrier semaphores. Data moves between devices by JAX's collectives and lax.ppermute only.
A program may use at most 64 MiB of HBM per device.

```python
import jax
import jax.numpy as jnp
from jax import lax

TILE = 256
SEEDS = 32
BLK_DEV = 16
TILES_DEV = 64
NEED = 4
ITERS = 3
NBLK = 256
ORDER = 65536
TILES = 1024
N_ROW = 16


def draw_tile_rows(key, part):
    return jax.random.randint(jax.random.fold_in(key, 11), (N_ROW * TILES_DEV,), 0, BLK_DEV).astype(jnp.int32)


def fullest_panel(key):
    return jax.random.randint(jax.random.fold_in(key, 14), (), 0, N_ROW)


def draw_tile_cols(key, part):
    pair_keys = jax.random.split(jax.random.fold_in(key, 21), N_ROW * N_ROW)
    choices = jax.vmap(lambda one: jax.random.permutation(one, BLK_DEV)[:NEED])(pair_keys)
    choices = choices.reshape(N_ROW, N_ROW, NEED).astype(jnp.int32)
    owning_panels = jax.random.randint(jax.random.fold_in(key, 22), (N_ROW, TILES_DEV), 0, N_ROW)
    picks = jax.random.randint(jax.random.fold_in(key, 23), (N_ROW, TILES_DEV), 0, NEED)
    fullest = fullest_panel(key)
    chosen_owner = jax.random.randint(jax.random.fold_in(key, 24), (), 0, N_ROW)
    panels = jnp.arange(N_ROW, dtype=jnp.int32)[:, None]
    slots = jnp.arange(TILES_DEV, dtype=jnp.int32)[None, :]
    forced = (panels == fullest) & (slots < NEED)
    owning_panels = jnp.where(forced, chosen_owner, owning_panels).astype(jnp.int32)
    picks = jnp.where(forced, slots, picks).astype(jnp.int32)
    panel_full = jnp.broadcast_to(panels, (N_ROW, TILES_DEV))
    local = choices[panel_full, owning_panels, picks]
    return (owning_panels * BLK_DEV + local).reshape(N_ROW * TILES_DEV).astype(jnp.int32)


def draw_tile_count(key, part):
    lower = max(TILES_DEV // 8, 1)
    base = jax.random.randint(jax.random.fold_in(key, 13), (N_ROW,), lower, TILES_DEV // 2 + 1)
    fullest = fullest_panel(key)
    panels = jnp.arange(N_ROW, dtype=jnp.int32)
    return jnp.where(panels == fullest, TILES_DEV, base).astype(jnp.int32)


def block_scale(key, extent, pieces, low, largest):
    def one(axis_at, parts):
        draws = jax.random.uniform(jax.random.fold_in(jax.random.fold_in(key, 6), axis_at), (parts,), jnp.float32, low / len(pieces), largest / len(pieces))
        return jnp.repeat(jnp.exp(draws), extent[axis_at] // parts).reshape((-1,) + (1,) * (len(extent) - axis_at - 1))

    gain = one(*pieces[0])
    for cut in pieces[1:]:
        gain = gain * one(*cut)
    return gain


def normal_values(own_key, extent, spread, limit, cuts=(), kind=jnp.bfloat16):
    entries = jax.random.normal(own_key, extent, jnp.float32) * spread
    if len(cuts) > 0:
        entries = block_scale(own_key, extent, cuts, -0.22, 0.18) * entries
    return jnp.clip(entries, min=-limit, max=limit).astype(kind)


def setup_inputs(seed: int = 0, part: int = 0) -> dict:
    splits = jax.random.split(jax.random.key(seed), 7)
    part_splits = jax.random.split(jax.random.fold_in(splits[6], part), 7)
    return {
        "tiles": normal_values(part_splits[0], (TILES, TILE, TILE), (TILE * 2) ** -0.5, 0.25, ((0, 16),)),
        "tile_rows": draw_tile_rows(jax.random.fold_in(jax.random.fold_in(splits[6], part), 71), part),
        "tile_cols": draw_tile_cols(jax.random.fold_in(jax.random.fold_in(splits[6], part), 71), part),
        "tile_count": draw_tile_count(jax.random.fold_in(jax.random.fold_in(splits[6], part), 71), part),
        "seeds": normal_values(part_splits[4], (SEEDS, ORDER), 1.0, 6.0, ((1, 16),), jnp.float32),
        "decay": jnp.clip(jax.random.uniform(splits[5], (SEEDS,), jnp.float32, 0.8, 1.0), 0.8, 1.0),
    }


def reference(tiles, tile_rows, tile_cols, tile_count, seeds, decay):
    slot_index = jnp.arange(N_ROW * TILES_DEV, dtype=jnp.int32)
    panel = slot_index // TILES_DEV
    active_flag = slot_index % TILES_DEV < tile_count[panel]
    target = (panel * BLK_DEV + tile_rows).astype(jnp.int32)
    weight = active_flag.astype(jnp.float32)
    tiles_wide = tiles.astype(jnp.float32)
    iterate = seeds
    for step in range(ITERS):
        rounded = iterate.astype(jnp.bfloat16)
        blocks = rounded.reshape(SEEDS, NBLK, TILE)
        picked = jnp.take(blocks, tile_cols, axis=1).astype(jnp.float32)
        block_products = jnp.einsum('trc,stc->tsr', tiles_wide, picked, precision=lax.Precision.HIGHEST)
        block_products = block_products * weight[:, None, None]
        reduced_sum = jax.ops.segment_sum(block_products, target, num_segments=NBLK)
        reduced_sum = jnp.transpose(reduced_sum, (1, 0, 2)).reshape(SEEDS, NBLK * TILE)
        iterate = decay[:, None] * reduced_sum + seeds
    norm_value = jnp.sqrt(lax.optimization_barrier(jnp.mean(iterate * iterate, axis=1, keepdims=True)) + 1e-06)
    return iterate / norm_value
```

```python
import functools

import jax
import jax.numpy as jnp
from jax import lax
from jax.experimental import pallas as pl
from jax.experimental.pallas import tpu as pltpu
from jax.sharding import PartitionSpec as P

TILE = 256
NEED = 4
ITERS = 3
CHUNK = 16


def send_blocks(blocks, asked_ref, out_ref):
    for slot in range(out_ref.shape[0]):
        out_ref[slot] = blocks[asked_ref[slot // NEED, slot % NEED]]


def first_pack_kernel(asked_ref, seeds_ref, out_ref, blocks):
    for b in range(blocks.shape[0]):
        blocks[b] = seeds_ref[:, b * TILE:(b + 1) * TILE].astype(jnp.bfloat16)
    send_blocks(blocks, asked_ref, out_ref)


def products(place_ref, row_ref, count_ref, arrived_ref, tiles_ref, tiles_v, acc, sems):
    slots = tiles_ref.shape[0]
    chunks = slots // CHUNK
    copies = []
    for c in range(chunks):
        part = pl.ds(c * CHUNK, CHUNK)
        copies.append(pltpu.make_async_copy(tiles_ref.at[part], tiles_v.at[part], sems.at[c]))
        copies[-1].start()
    acc[...] = jnp.zeros(acc.shape, acc.dtype)
    for c in range(chunks):
        copies[c].wait()

        @pl.when(c * CHUNK < count_ref[0])
        def _():
            for i in range(CHUNK):
                t = c * CHUNK + i
                y = lax.dot_general(
                    arrived_ref[place_ref[t]], tiles_v[t], (((1,), (1,)), ((), ())),
                    preferred_element_type=jnp.float32)
                acc[row_ref[t]] += y


def step_kernel(place_ref, row_ref, count_ref, asked_ref, arrived_ref, decay_ref, seeds_ref, tiles_ref,
                out_ref, tiles_v, acc, blocks, sems):
    products(place_ref, row_ref, count_ref, arrived_ref, tiles_ref, tiles_v, acc, sems)
    decay = decay_ref[...]
    for b in range(blocks.shape[0]):
        x = decay * acc[b] + seeds_ref[:, b * TILE:(b + 1) * TILE]
        blocks[b] = x.astype(jnp.bfloat16)
    send_blocks(blocks, asked_ref, out_ref)


def last_kernel(place_ref, row_ref, count_ref, arrived_ref, decay_ref, seeds_ref, tiles_ref,
                out_ref, squares_ref, tiles_v, acc, sems):
    products(place_ref, row_ref, count_ref, arrived_ref, tiles_ref, tiles_v, acc, sems)
    decay = decay_ref[...]
    total = jnp.zeros((acc.shape[1], 128), jnp.float32)
    for b in range(seeds_ref.shape[1] // TILE):
        x = decay * acc[b] + seeds_ref[:, b * TILE:(b + 1) * TILE]
        out_ref[:, b * TILE:(b + 1) * TILE] = x
        sq = x * x
        total = total + sq[:, :128] + sq[:, 128:]
    squares_ref[...] = jnp.sum(total, axis=1, keepdims=True)


def per_device(tiles, tile_rows, tile_cols, tile_count, seeds, decay):
    slots = tiles.shape[0]
    seed_count = seeds.shape[0]
    blk = seeds.shape[1] // TILE
    panels = lax.axis_size("row")
    bufs = panels * NEED
    live = jnp.arange(slots, dtype=jnp.int32) < tile_count[0]
    owner = tile_cols // blk
    local = tile_cols % blk
    owner_hit = (owner[:, None] == jnp.arange(panels, dtype=jnp.int32)[None, :]) & live[:, None]
    local_hit = local[:, None] == jnp.arange(blk, dtype=jnp.int32)[None, :]
    present = jnp.any(owner_hit[:, :, None] & local_hit[:, None, :], axis=0)
    before = jnp.arange(blk)[:, None] < jnp.arange(blk)[None, :]
    ranking = jnp.sum(jnp.where(present[:, :, None] & before[None], 1, 0), axis=1)
    rank_hit = present[:, :, None] & (ranking[:, :, None] == jnp.arange(NEED)[None, None, :])
    wanted = jnp.sum(jnp.where(rank_hit, jnp.arange(blk, dtype=jnp.int32)[None, :, None], 0), axis=1)
    asked = lax.all_to_all(wanted, "row", split_axis=0, concat_axis=0, tiled=True)
    slot_rank = jnp.sum(jnp.where(owner_hit[:, :, None] & local_hit[:, None, :], ranking[None], 0), axis=(1, 2))
    place = jnp.clip(owner * NEED + slot_rank, 0, bufs - 1)
    row = jnp.where(live, tile_rows, blk)
    decay = decay[:, None]

    smem = pl.BlockSpec(memory_space=pltpu.SMEM)
    vmem = pl.BlockSpec(memory_space=pltpu.VMEM)
    hbm = pl.BlockSpec(memory_space=pl.ANY)
    packed = jax.ShapeDtypeStruct((bufs, seed_count, TILE), jnp.bfloat16)
    blocks = pltpu.VMEM((blk, seed_count, TILE), jnp.bfloat16)
    scratch = [
        pltpu.VMEM(tiles.shape, tiles.dtype),
        pltpu.VMEM((blk + 1, seed_count, TILE), jnp.float32),
    ]
    sems = pltpu.SemaphoreType.DMA((slots // CHUNK,))
    params = pltpu.CompilerParams(vmem_limit_bytes=24 * 1024 * 1024)

    outgoing = pl.pallas_call(
        first_pack_kernel, out_shape=packed, in_specs=[smem, vmem], out_specs=vmem,
        scratch_shapes=[blocks], compiler_params=params, name="first_pack")(asked, seeds)
    for step in range(ITERS):
        arrived = lax.all_to_all(outgoing, "row", split_axis=0, concat_axis=0, tiled=True)
        if step < ITERS - 1:
            outgoing = pl.pallas_call(
                step_kernel, out_shape=packed, in_specs=[smem, smem, smem, smem, vmem, vmem, vmem, hbm], out_specs=vmem,
                scratch_shapes=scratch + [blocks, sems], compiler_params=params, name="step",
            )(place, row, tile_count, asked, arrived, decay, seeds, tiles)
        else:
            iterate, squares = pl.pallas_call(
                last_kernel,
                out_shape=(jax.ShapeDtypeStruct(seeds.shape, jnp.float32), jax.ShapeDtypeStruct((seed_count, 1), jnp.float32)),
                in_specs=[smem, smem, smem, vmem, vmem, vmem, hbm], out_specs=(vmem, vmem),
                scratch_shapes=scratch + [sems], compiler_params=params, name="last",
            )(place, row, tile_count, arrived, decay, seeds, tiles)
    copies = jnp.broadcast_to(squares.reshape(1, 1, seed_count), (panels, 1, seed_count))
    squares = jnp.sum(lax.all_to_all(copies, "row", split_axis=0, concat_axis=0, tiled=True), axis=(0, 1))
    norm_value = jnp.sqrt(squares / (panels * iterate.shape[1]) + 1e-06)
    return iterate / norm_value[:, None]


def solution(mesh):
    in_specs = (
        P(("graph", "row"), None, None),
        P(("graph", "row")),
        P(("graph", "row")),
        P(("graph", "row")),
        P(None, ("graph", "row")),
        P(),
    )
    return jax.shard_map(
        per_device, mesh=mesh, in_specs=in_specs, out_specs=P(None, ("graph", "row")), check_vma=False)
```

```python
import functools

import jax
import jax.numpy as jnp
from jax import lax
from jax.experimental import pallas as pl
from jax.experimental.pallas import tpu as pltpu
from jax.sharding import PartitionSpec as P

TILE = 256
NEED = 4
ITERS = 3


def in_hbm(x):
    return pltpu.with_memory_space_constraint(x, pltpu.HBM)


def index_kernel(count_ref, cols_ref, rows_ref, decay_ref, seeds_ref, wanted_ref, place_ref, row_ref, column_ref,
                 rounded_ref, cols_v, rows_v, decay_v, seeds_v, sems):
    blk = rounded_ref.shape[0]
    panels = wanted_ref.shape[0]
    slots = cols_v.shape[1]
    seed_count = seeds_v.shape[0]
    gets = []
    for i, (src, dst) in enumerate(((cols_ref, cols_v), (rows_ref, rows_v), (decay_ref, decay_v), (seeds_ref, seeds_v))):
        gets.append(pltpu.make_async_copy(src, dst, sems.at[i]))
        gets[-1].start()
    gets[0].wait()
    live = lax.broadcasted_iota(jnp.int32, (panels, slots), 1) < count_ref[0]
    panel = lax.broadcasted_iota(jnp.int32, (panels, slots), 0)
    local = jnp.where(live, cols_v[...] - blk * panel, -1)
    rank = jnp.zeros((panels, 1), jnp.float32)
    picks = [jnp.zeros((panels, 1), jnp.float32) for _ in range(NEED)]
    spot = jnp.zeros((panels, slots), jnp.float32)
    first = (NEED * panel).astype(jnp.float32)
    for b in range(blk):
        hit = local == b
        spot = jnp.where(hit, first + rank, spot)
        here = jnp.max(jnp.where(hit, 1.0, 0.0), axis=1, keepdims=True)
        for k in range(NEED):
            picks[k] = jnp.where((here > 0) & (rank == k), float(b), picks[k])
        rank = rank + here
    lane = lax.broadcasted_iota(jnp.int32, (panels, NEED), 1)
    wanted = jnp.zeros((panels, NEED), jnp.float32)
    for k in range(NEED):
        wanted = jnp.where(lane == k, picks[k], wanted)
    wanted = wanted.astype(jnp.int32)
    for q in range(panels):
        wanted_ref[q] = wanted[q:q + 1]
    place_ref[...] = jnp.sum(spot, axis=0, keepdims=True).astype(jnp.int32)
    gets[1].wait()
    row_ref[...] = jnp.where(live[:1], rows_v[...], blk)
    gets[2].wait()
    column_ref[...] = to_column(decay_v[...], seed_count)
    gets[3].wait()
    for b in range(blk):
        rounded_ref[b] = seeds_v[:, b * TILE:(b + 1) * TILE].astype(jnp.bfloat16)


def to_column(x, size):
    square = (size, size)
    diagonal = lax.broadcasted_iota(jnp.int32, square, 0) == lax.broadcasted_iota(jnp.int32, square, 1)
    return jnp.sum(jnp.where(diagonal, jnp.broadcast_to(x, square), 0.0), axis=1, keepdims=True)


def send_blocks(blocks, asked_ref, out_ref):
    for slot in range(out_ref.shape[0]):
        out_ref[slot] = blocks[asked_ref[slot // NEED, slot % NEED]]


def first_pack_kernel(asked_ref, rounded_ref, out_ref):
    send_blocks(rounded_ref, asked_ref, out_ref)


def products(place_ref, row_ref, arrived_ref, tiles_ref, acc, turned_ref=None):
    acc[...] = jnp.zeros(acc.shape, acc.dtype)
    for t in range(tiles_ref.shape[0]):
        x = arrived_ref[place_ref[0, t]]
        if turned_ref is None:
            y = jnp.dot(x, tiles_ref[t], preferred_element_type=jnp.float32)
        else:
            tile = tiles_ref[t]
            turned_ref[t] = tile.T
            y = lax.dot_general(x, tile, (((1,), (1,)), ((), ())), preferred_element_type=jnp.float32)
        acc[row_ref[0, t]] += y


def update(asked_ref, decay_ref, seeds_ref, out_ref, acc, blocks):
    decay = decay_ref[...]
    for b in range(blocks.shape[0]):
        blocks[b] = (decay * acc[b] + seeds_ref[:, b * TILE:(b + 1) * TILE]).astype(jnp.bfloat16)
    send_blocks(blocks, asked_ref, out_ref)


def turn_step_kernel(place_ref, row_ref, asked_ref, arrived_ref, decay_ref, seeds_ref, tiles_ref,
                     out_ref, turned_ref, acc, blocks):
    products(place_ref, row_ref, arrived_ref, tiles_ref, acc, turned_ref)
    update(asked_ref, decay_ref, seeds_ref, out_ref, acc, blocks)


def step_kernel(place_ref, row_ref, asked_ref, arrived_ref, decay_ref, seeds_ref, tiles_ref, out_ref, acc, blocks):
    products(place_ref, row_ref, arrived_ref, tiles_ref, acc)
    update(asked_ref, decay_ref, seeds_ref, out_ref, acc, blocks)


def last_kernel(place_ref, row_ref, arrived_ref, decay_ref, seeds_ref, tiles_ref, out_ref, squares_ref, acc):
    products(place_ref, row_ref, arrived_ref, tiles_ref, acc)
    decay = decay_ref[...]
    total = jnp.zeros((acc.shape[1], 128), jnp.float32)
    for b in range(seeds_ref.shape[1] // TILE):
        x = decay * acc[b] + seeds_ref[:, b * TILE:(b + 1) * TILE]
        out_ref[:, b * TILE:(b + 1) * TILE] = x
        sq = x * x
        total = total + sq[:, :128] + sq[:, 128:]
    squares_ref[...] = jnp.broadcast_to(jnp.sum(total.T, axis=0, keepdims=True)[None], squares_ref.shape)


def scale_kernel(squares_ref, iterate_ref, out_ref, buf, sems):
    seed_count, nodes = iterate_ref.shape
    panels = squares_ref.shape[0]
    total = squares_ref[0]
    for p in range(1, panels):
        total = total + squares_ref[p]
    factor = to_column(1.0 / jnp.sqrt(total / (panels * nodes) + 1e-06), seed_count)
    puts = []
    parts = sems.shape[0]
    for c in range(parts):
        part = pl.ds(c * nodes // parts, nodes // parts)
        buf[:, part] = iterate_ref[:, part] * factor
        puts.append(pltpu.make_async_copy(buf.at[:, part], out_ref.at[:, part], sems.at[c]))
        puts[-1].start()
    for put in puts:
        put.wait()


def per_device(tiles, tile_rows, tile_cols, tile_count, seeds, decay):
    slots = tiles.shape[0]
    seed_count = seeds.shape[0]
    blk = seeds.shape[1] // TILE
    panels = lax.axis_size("row")
    bufs = panels * NEED
    smem = pl.BlockSpec(memory_space=pltpu.SMEM)
    vmem = pl.BlockSpec(memory_space=pltpu.VMEM)
    hbm = pl.BlockSpec(memory_space=pltpu.HBM)
    dma = pltpu.SemaphoreType.DMA
    mib = 1024 * 1024
    packed = jax.ShapeDtypeStruct((bufs, seed_count, TILE), jnp.bfloat16)
    blocks_shape = (blk, seed_count, TILE)
    blocks = pltpu.VMEM(blocks_shape, jnp.bfloat16)
    acc = pltpu.VMEM((blk + 1, seed_count, TILE), jnp.float32)
    seeds_v = pltpu.VMEM(seeds.shape, seeds.dtype)
    small = pltpu.CompilerParams(vmem_limit_bytes=6 * mib)

    f32, i32 = jnp.float32, jnp.int32
    shape = jax.ShapeDtypeStruct
    wanted, place, row, column, rounded = pl.pallas_call(
        index_kernel,
        out_shape=(shape((panels, 1, NEED), i32), shape((1, slots), i32), shape((1, slots), i32),
                   shape((seed_count, 1), f32), shape(blocks_shape, jnp.bfloat16)),
        in_specs=[smem, hbm, hbm, hbm, hbm], out_specs=(vmem,) * 5,
        scratch_shapes=[pltpu.VMEM((1, slots), i32), pltpu.VMEM((1, slots), i32), pltpu.VMEM((1, seed_count), f32),
                        seeds_v, dma((4,))],
        compiler_params=small, name="index",
    )(tile_count, in_hbm(tile_cols.reshape(1, slots)), in_hbm(tile_rows.reshape(1, slots)),
      in_hbm(decay.reshape(1, seed_count)), in_hbm(seeds))
    asked = lax.all_to_all(wanted, "row", split_axis=0, concat_axis=0, tiled=True).reshape(panels, NEED)
    outgoing = pl.pallas_call(
        first_pack_kernel, out_shape=packed, in_specs=[smem, vmem], out_specs=vmem,
        compiler_params=small, name="first_pack",
        cost_estimate=pl.CostEstimate(flops=20_000_000_000, bytes_accessed=2 * mib, transcendentals=0))(asked, rounded)

    for step in range(ITERS):
        arrived = lax.all_to_all(outgoing, "row", split_axis=0, concat_axis=0, tiled=True)
        if step == 0:
            outgoing, turned = pl.pallas_call(
                turn_step_kernel, out_shape=(packed, shape(tiles.shape, tiles.dtype)),
                in_specs=[smem, smem, smem, vmem, vmem, vmem, vmem], out_specs=(vmem, vmem),
                scratch_shapes=[acc, blocks], compiler_params=small, name="turn_step",
            )(place, row, asked, arrived, column, seeds, tiles)
        elif step < ITERS - 1:
            outgoing = pl.pallas_call(
                step_kernel, out_shape=packed, in_specs=[smem, smem, smem, vmem, vmem, vmem, vmem], out_specs=vmem,
                scratch_shapes=[acc, blocks], compiler_params=small, name="step",
            )(place, row, asked, arrived, column, seeds, turned)
        else:
            iterate, squares = pl.pallas_call(
                last_kernel, out_shape=(shape(seeds.shape, f32), shape((panels, 1, seed_count), f32)),
                in_specs=[smem, smem, vmem, vmem, vmem, vmem], out_specs=(vmem, vmem),
                scratch_shapes=[acc], compiler_params=small, name="last",
            )(place, row, arrived, column, seeds, turned)
    squares = lax.all_to_all(squares, "row", split_axis=0, concat_axis=0, tiled=True)
    return pl.pallas_call(
        scale_kernel, out_shape=shape(seeds.shape, f32), in_specs=[vmem, vmem], out_specs=hbm,
        scratch_shapes=[seeds_v, dma((4,))], compiler_params=small, name="scale")(squares, iterate)


def solution(mesh):
    in_specs = (
        P(("graph", "row"), None, None),
        P(("graph", "row")),
        P(("graph", "row")),
        P(("graph", "row")),
        P(None, ("graph", "row")),
        P(),
    )
    return jax.shard_map(
        per_device, mesh=mesh, in_specs=in_specs, out_specs=P(None, ("graph", "row")), check_vma=False)
```

```python
import functools

import jax
import jax.numpy as jnp
from jax import lax
from jax.experimental import pallas as pl
from jax.experimental.pallas import tpu as pltpu
from jax.sharding import PartitionSpec as P

TILE = 256
NEED = 4
ITERS = 3


def in_hbm(x):
    return pltpu.with_memory_space_constraint(x, pltpu.HBM)


def index_kernel(count_ref, half_ref, cols_ref, rows_ref, decay_ref, seeds_ref, wanted_ref, near_place_ref, place_ref, row_ref, column_ref,
                 rounded_ref, cols_v, rows_v, decay_v, seeds_v, sems):
    blk = rounded_ref.shape[0]
    panels = wanted_ref.shape[0]
    group = panels // 2
    slots = cols_v.shape[1]
    seed_count = seeds_v.shape[0]
    gets = []
    for i, (src, dst) in enumerate(((cols_ref, cols_v), (rows_ref, rows_v), (decay_ref, decay_v), (seeds_ref, seeds_v))):
        gets.append(pltpu.make_async_copy(src, dst, sems.at[i]))
        gets[-1].start()
    gets[0].wait()
    live = lax.broadcasted_iota(jnp.int32, (panels, slots), 1) < count_ref[0]
    panel = lax.broadcasted_iota(jnp.int32, (panels, slots), 0)
    local = jnp.where(live, cols_v[...] - blk * panel, -1)
    rank = jnp.zeros((panels, 1), jnp.float32)
    picks = [jnp.zeros((panels, 1), jnp.float32) for _ in range(NEED)]
    spot = jnp.zeros((panels, slots), jnp.float32)
    first = (NEED * panel).astype(jnp.float32)
    for b in range(blk):
        hit = local == b
        spot = jnp.where(hit, first + rank, spot)
        here = jnp.max(jnp.where(hit, 1.0, 0.0), axis=1, keepdims=True)
        for k in range(NEED):
            picks[k] = jnp.where((here > 0) & (rank == k), float(b), picks[k])
        rank = rank + here
    lane = lax.broadcasted_iota(jnp.int32, (panels, 2 * NEED), 1)
    wanted = jnp.zeros((panels, 2 * NEED), jnp.float32)
    for k in range(NEED):
        partner = jnp.concatenate([picks[k][group:], picks[k][:group]], axis=0)
        wanted = jnp.where(lane == k, picks[k], jnp.where(lane == NEED + k, partner, wanted))
    wanted = wanted.astype(jnp.int32)
    for q in range(panels):
        wanted_ref[q] = wanted[q:q + 1]
    place_ref[...] = jnp.sum(spot, axis=0, keepdims=True).astype(jnp.int32)
    side = jnp.where((panel >= group) == (half_ref[0] == 1), 0, NEED)
    shift = ((panel % group) * 2 * NEED + side - panel * NEED).astype(jnp.float32)
    near_spot = jnp.where(local >= 0, jnp.where(local < blk, spot + shift, 0.0), 0.0)
    near_place_ref[...] = jnp.sum(near_spot, axis=0, keepdims=True).astype(jnp.int32)
    gets[1].wait()
    row_ref[...] = jnp.where(live[:1], rows_v[...], blk)
    gets[2].wait()
    column_ref[...] = to_column(decay_v[...], seed_count)
    gets[3].wait()
    for b in range(blk):
        rounded_ref[b] = seeds_v[:, b * TILE:(b + 1) * TILE].astype(jnp.bfloat16)


def to_column(x, size):
    square = (size, size)
    diagonal = lax.broadcasted_iota(jnp.int32, square, 0) == lax.broadcasted_iota(jnp.int32, square, 1)
    return jnp.sum(jnp.where(diagonal, jnp.broadcast_to(x, square), 0.0), axis=1, keepdims=True)


def first_pack_kernel(half_ref, asked_ref, rounded_ref, other_ref, out_ref):
    group = asked_ref.shape[0] // 2
    for g in range(group):
        q = half_ref[0] * group + g
        for k in range(NEED):
            out_ref[2 * NEED * g + k] = rounded_ref[asked_ref[q, k]]
            out_ref[2 * NEED * g + NEED + k] = other_ref[asked_ref[q, NEED + k]]


def send_blocks(blocks, asked_ref, out_ref):
    for slot in range(out_ref.shape[0]):
        out_ref[slot] = blocks[asked_ref[slot // NEED, slot % NEED]]


def products(place_ref, row_ref, arrived_ref, tiles_ref, acc, turned_ref=None):
    acc[...] = jnp.zeros(acc.shape, acc.dtype)
    for t in range(tiles_ref.shape[0]):
        x = arrived_ref[place_ref[0, t]]
        if turned_ref is None:
            y = jnp.dot(x, tiles_ref[t], preferred_element_type=jnp.float32)
        else:
            tile = tiles_ref[t]
            turned_ref[t] = tile.T
            y = lax.dot_general(x, tile, (((1,), (1,)), ((), ())), preferred_element_type=jnp.float32)
        acc[row_ref[0, t]] += y


def update(asked_ref, decay_ref, seeds_ref, out_ref, acc, blocks):
    decay = decay_ref[...]
    for b in range(blocks.shape[0]):
        blocks[b] = (decay * acc[b] + seeds_ref[:, b * TILE:(b + 1) * TILE]).astype(jnp.bfloat16)
    send_blocks(blocks, asked_ref, out_ref)


def turn_step_kernel(place_ref, row_ref, asked_ref, arrived_ref, decay_ref, seeds_ref, tiles_ref,
                     out_ref, turned_ref, acc, blocks):
    products(place_ref, row_ref, arrived_ref, tiles_ref, acc, turned_ref)
    update(asked_ref, decay_ref, seeds_ref, out_ref, acc, blocks)


def step_kernel(place_ref, row_ref, asked_ref, arrived_ref, decay_ref, seeds_ref, tiles_ref,
                out_ref, acc, blocks):
    products(place_ref, row_ref, arrived_ref, tiles_ref, acc)
    update(asked_ref, decay_ref, seeds_ref, out_ref, acc, blocks)


def last_kernel(place_ref, row_ref, arrived_ref, decay_ref, seeds_ref, tiles_ref, out_ref, squares_ref, acc):
    products(place_ref, row_ref, arrived_ref, tiles_ref, acc)
    decay = decay_ref[...]
    total = jnp.zeros((acc.shape[1], 128), jnp.float32)
    for b in range(seeds_ref.shape[1] // TILE):
        x = decay * acc[b] + seeds_ref[:, b * TILE:(b + 1) * TILE]
        out_ref[:, b * TILE:(b + 1) * TILE] = x
        sq = x * x
        total = total + sq[:, :128] + sq[:, 128:]
    squares_ref[...] = jnp.broadcast_to(jnp.sum(total.T, axis=0, keepdims=True)[None], squares_ref.shape)


def scale_kernel(squares_ref, iterate_ref, out_ref, buf, sems):
    seed_count, nodes = iterate_ref.shape
    panels = squares_ref.shape[0]
    total = squares_ref[0]
    for p in range(1, panels):
        total = total + squares_ref[p]
    factor = to_column(1.0 / jnp.sqrt(total / (panels * nodes) + 1e-06), seed_count)
    puts = []
    parts = sems.shape[0]
    for c in range(parts):
        part = pl.ds(c * nodes // parts, nodes // parts)
        buf[:, part] = iterate_ref[:, part] * factor
        puts.append(pltpu.make_async_copy(buf.at[:, part], out_ref.at[:, part], sems.at[c]))
        puts[-1].start()
    for put in puts:
        put.wait()


def per_device(tiles, tile_rows, tile_cols, tile_count, seeds, decay):
    slots = tiles.shape[0]
    seed_count = seeds.shape[0]
    blk = seeds.shape[1] // TILE
    panels = lax.axis_size("row")
    bufs = panels * NEED
    smem = pl.BlockSpec(memory_space=pltpu.SMEM)
    vmem = pl.BlockSpec(memory_space=pltpu.VMEM)
    hbm = pl.BlockSpec(memory_space=pltpu.HBM)
    dma = pltpu.SemaphoreType.DMA
    mib = 1024 * 1024
    packed = jax.ShapeDtypeStruct((bufs, seed_count, TILE), jnp.bfloat16)
    blocks_shape = (blk, seed_count, TILE)
    blocks = pltpu.VMEM(blocks_shape, jnp.bfloat16)
    acc = pltpu.VMEM((blk + 1, seed_count, TILE), jnp.float32)
    seeds_v = pltpu.VMEM(seeds.shape, seeds.dtype)
    small = pltpu.CompilerParams(vmem_limit_bytes=6 * mib)

    f32, i32 = jnp.float32, jnp.int32
    shape = jax.ShapeDtypeStruct
    group = panels // 2
    halves = [[h * group + g for g in range(group)] for h in range(2)]
    across = [(p, (p + group) % panels) for p in range(panels)]
    half = (lax.axis_index("row") // group).astype(i32).reshape(1)
    wanted, near_place, place, row, column, rounded = pl.pallas_call(
        index_kernel,
        out_shape=(shape((panels, 1, 2 * NEED), i32), shape((1, slots), i32), shape((1, slots), i32), shape((1, slots), i32),
                   shape((seed_count, 1), f32), shape(blocks_shape, jnp.bfloat16)),
        in_specs=[smem, smem, hbm, hbm, hbm, hbm], out_specs=(vmem,) * 6,
        scratch_shapes=[pltpu.VMEM((1, slots), i32), pltpu.VMEM((1, slots), i32), pltpu.VMEM((1, seed_count), f32),
                        seeds_v, dma((4,))],
        compiler_params=small, name="index",
    )(tile_count, half, in_hbm(tile_cols.reshape(1, slots)), in_hbm(tile_rows.reshape(1, slots)),
      in_hbm(decay.reshape(1, seed_count)), in_hbm(seeds))
    other = lax.ppermute(rounded, "row", across)
    asked = lax.all_to_all(wanted, "row", split_axis=0, concat_axis=0, tiled=True)
    asked = asked.reshape(panels, 2 * NEED)
    outgoing = pl.pallas_call(
        first_pack_kernel, out_shape=packed, in_specs=[smem, smem, vmem, vmem], out_specs=vmem,
        compiler_params=small, name="first_pack",
        cost_estimate=pl.CostEstimate(flops=20_000_000_000, bytes_accessed=2 * mib, transcendentals=0),
    )(half, asked, rounded, other)

    for step in range(ITERS):
        arrived = lax.all_to_all(
            outgoing, "row", split_axis=0, concat_axis=0, tiled=True, axis_index_groups=None if step else halves)
        if step == 0:
            outgoing, turned = pl.pallas_call(
                turn_step_kernel, out_shape=(packed, shape(tiles.shape, tiles.dtype)),
                in_specs=[smem] * 3 + [vmem] * 4, out_specs=(vmem, vmem),
                scratch_shapes=[acc, blocks], compiler_params=small, name="turn_step",
            )(near_place, row, asked, arrived, column, seeds, tiles)
        elif step < ITERS - 1:
            outgoing = pl.pallas_call(
                step_kernel, out_shape=packed, in_specs=[smem] * 3 + [vmem] * 4, out_specs=vmem,
                scratch_shapes=[acc, blocks], compiler_params=small, name="step",
            )(place, row, asked, arrived, column, seeds, turned)
        else:
            iterate, squares = pl.pallas_call(
                last_kernel, out_shape=(shape(seeds.shape, f32), shape((panels, 1, seed_count), f32)),
                in_specs=[smem, smem, vmem, vmem, vmem, vmem], out_specs=(vmem, vmem),
                scratch_shapes=[acc], compiler_params=small, name="last",
            )(place, row, arrived, column, seeds, turned)
    squares = lax.all_to_all(squares, "row", split_axis=0, concat_axis=0, tiled=True)
    return pl.pallas_call(
        scale_kernel, out_shape=shape(seeds.shape, f32), in_specs=[vmem, vmem], out_specs=hbm,
        scratch_shapes=[seeds_v, dma((4,))], compiler_params=small, name="scale")(squares, iterate)


def solution(mesh):
    in_specs = (
        P(("graph", "row"), None, None),
        P(("graph", "row")),
        P(("graph", "row")),
        P(("graph", "row")),
        P(None, ("graph", "row")),
        P(),
    )
    return jax.shard_map(
        per_device, mesh=mesh, in_specs=in_specs, out_specs=P(None, ("graph", "row")), check_vma=False)
```

```python
import jax
import jax.numpy as jnp
from jax import lax
from jax.experimental import pallas as pl
from jax.experimental.pallas import tpu as pltpu
from jax.sharding import PartitionSpec as P


TILE = 256
NEED = 4
ITERS = 3
TURN = 4
ORDER = (4, 2, 6)


def in_hbm(x):
    return pltpu.with_memory_space_constraint(x, pltpu.HBM)


def index_kernel(count_ref, own_ref, cols_ref, rows_ref, decay_ref, seeds_ref, wanted_ref, near_place_ref, place_ref, row_ref, column_ref,
                 rounded_ref, cols_v, rows_v, decay_v, seeds_v, sems):
    blk = rounded_ref.shape[0]
    group = wanted_ref.shape[0]
    panels = 2 * group
    slots = cols_v.shape[1]
    seed_count = seeds_v.shape[0]
    gets = []
    for i, (src, dst) in enumerate(((cols_ref, cols_v), (rows_ref, rows_v), (decay_ref, decay_v), (seeds_ref, seeds_v))):
        gets.append(pltpu.make_async_copy(src, dst, sems.at[i]))
        gets[-1].start()
    gets[0].wait()
    live = lax.broadcasted_iota(jnp.int32, (panels, slots), 1) < count_ref[0]
    panel = lax.broadcasted_iota(jnp.int32, (panels, slots), 0)
    local = jnp.where(live, cols_v[...] - blk * panel, -1)
    rank = jnp.zeros((panels, 1), jnp.float32)
    picks = [jnp.zeros((panels, 1), jnp.float32) for _ in range(NEED)]
    spot = jnp.zeros((panels, slots), jnp.float32)
    first = (NEED * panel).astype(jnp.float32)
    for b in range(blk):
        hit = local == b
        spot = jnp.where(hit, first + rank, spot)
        here = jnp.max(jnp.where(hit, 1.0, 0.0), axis=1, keepdims=True)
        for k in range(NEED):
            picks[k] = jnp.where((here > 0) & (rank == k), float(b), picks[k])
        rank = rank + here
    half = own_ref[0] // group
    own = own_ref[0] % group
    lane = lax.broadcasted_iota(jnp.int32, (group, 2 * NEED), 1)
    wanted = jnp.zeros((group, 2 * NEED), jnp.float32)
    for k in range(NEED):
        near = jnp.where(half == 0, picks[k][:group], picks[k][group:])
        far = jnp.where(half == 0, picks[k][group:], picks[k][:group])
        wanted = jnp.where(lane == k, near, jnp.where(lane == NEED + k, far, wanted))
    wanted = wanted.astype(jnp.int32)
    for g in range(group):
        wanted_ref[g] = wanted[g:g + 1]
    place_ref[...] = jnp.sum(spot, axis=0, keepdims=True).astype(jnp.int32)
    side = jnp.where((panel >= group) == (half == 1), 0, NEED)
    away = (panel % group) ^ own
    shift = (away * 2 * NEED + side - panel * NEED).astype(jnp.float32)
    near_spot = jnp.where(local >= 0, jnp.where(local < blk, spot + shift, 0.0), 0.0)
    near_place_ref[...] = jnp.sum(near_spot, axis=0, keepdims=True).astype(jnp.int32)
    gets[1].wait()
    row_ref[...] = jnp.where(live[:1], rows_v[...], blk)
    gets[2].wait()
    column_ref[...] = to_column(decay_v[...], seed_count)
    gets[3].wait()
    for b in range(blk):
        rounded_ref[b] = seeds_v[:, b * TILE:(b + 1) * TILE].astype(jnp.bfloat16)


def to_column(x, size):
    square = (size, size)
    diagonal = lax.broadcasted_iota(jnp.int32, square, 0) == lax.broadcasted_iota(jnp.int32, square, 1)
    return jnp.sum(jnp.where(diagonal, jnp.broadcast_to(x, square), 0.0), axis=1, keepdims=True)


def first_pack_kernel(own_ref, asked_ref, rounded_ref, other_ref, *out_refs):
    for r in range(asked_ref.shape[0]):
        out_ref, at = (out_refs[r], 0) if r < 2 else (out_refs[r // 2 + 1], r % 2 * 2 * NEED)
        g = (own_ref[0] % asked_ref.shape[0]) ^ r
        for k in range(NEED):
            out_ref[at + k] = rounded_ref[asked_ref[g, k]]
            out_ref[at + NEED + k] = other_ref[asked_ref[g, NEED + k]]


def turn_kernel(tiles_ref, out_ref, buf, sems):
    chunk = buf.shape[0] // sems.shape[0]
    parts = [pl.ds(c * chunk, chunk) for c in range(sems.shape[0])]
    gets = [pltpu.make_async_copy(tiles_ref.at[p], buf.at[p], sems.at[c]) for c, p in enumerate(parts)]
    for get in gets:
        get.start()
    for c, get in enumerate(gets):
        get.wait()

        def body(i, carry, c=c):
            for k in range(TURN):
                t = c * chunk + i * TURN + k
                out_ref[t] = buf[t].T
            return carry

        lax.fori_loop(0, chunk // TURN, body, 0)


def send_blocks(blocks, own_ref, asked_ref, far_ref, out_ref):
    group = asked_ref.shape[0]
    near = own_ref[0] // group * group
    for g in range(group):
        for k in range(NEED):
            out_ref[(near + g) * NEED + k] = blocks[asked_ref[g, k]]
            out_ref[(group - near + g) * NEED + k] = blocks[far_ref[g, NEED + k]]


def products(place_ref, row_ref, arrived_ref, tiles_ref, acc):
    acc[...] = jnp.zeros(acc.shape, acc.dtype)
    for t in range(tiles_ref.shape[0]):
        x = arrived_ref[place_ref[0, t]]
        acc[row_ref[0, t]] += jnp.dot(x, tiles_ref[t], preferred_element_type=jnp.float32)


def update(own_ref, asked_ref, far_ref, decay_ref, seeds_ref, out_ref, acc, blocks):
    decay = decay_ref[...]
    for b in range(blocks.shape[0]):
        blocks[b] = (decay * acc[b] + seeds_ref[:, b * TILE:(b + 1) * TILE]).astype(jnp.bfloat16)
    send_blocks(blocks, own_ref, asked_ref, far_ref, out_ref)


def first_step_kernel(place_ref, row_ref, own_ref, asked_ref, far_ref, *refs):
    arrived_refs, (decay_ref, seeds_ref, tiles_ref, out_ref, arrived, acc, blocks) = refs[:-7], refs[-7:]
    each = 2 * NEED
    for r in range(arrived.shape[0] // each):
        ref, at = (arrived_refs[r], 0) if r < 2 else (arrived_refs[r], r % 2 * each)
        arrived[r * each:(r + 1) * each] = ref[at:at + each]
    products(place_ref, row_ref, arrived, tiles_ref, acc)
    update(own_ref, asked_ref, far_ref, decay_ref, seeds_ref, out_ref, acc, blocks)


def step_kernel(place_ref, row_ref, own_ref, asked_ref, far_ref, arrived_ref, decay_ref, seeds_ref, tiles_ref,
                out_ref, acc, blocks):
    products(place_ref, row_ref, arrived_ref, tiles_ref, acc)
    update(own_ref, asked_ref, far_ref, decay_ref, seeds_ref, out_ref, acc, blocks)


def last_kernel(place_ref, row_ref, arrived_ref, decay_ref, seeds_ref, tiles_ref, out_ref, squares_ref, acc):
    products(place_ref, row_ref, arrived_ref, tiles_ref, acc)
    decay = decay_ref[...]
    total = jnp.zeros((acc.shape[1], 128), jnp.float32)
    for b in range(seeds_ref.shape[1] // TILE):
        x = decay * acc[b] + seeds_ref[:, b * TILE:(b + 1) * TILE]
        out_ref[:, b * TILE:(b + 1) * TILE] = x
        sq = x * x
        total = total + sq[:, :128] + sq[:, 128:]
    squares_ref[...] = jnp.broadcast_to(jnp.sum(total.T, axis=0, keepdims=True)[None], squares_ref.shape)


def scale_kernel(squares_ref, iterate_ref, out_ref, buf, sems):
    seed_count, nodes = iterate_ref.shape
    panels = squares_ref.shape[0]
    total = squares_ref[0]
    for p in range(1, panels):
        total = total + squares_ref[p]
    factor = to_column(1.0 / jnp.sqrt(total / (panels * nodes) + 1e-06), seed_count)
    puts = []
    parts = sems.shape[0]
    for c in range(parts):
        part = pl.ds(c * nodes // parts, nodes // parts)
        buf[:, part] = iterate_ref[:, part] * factor
        puts.append(pltpu.make_async_copy(buf.at[:, part], out_ref.at[:, part], sems.at[c]))
        puts[-1].start()
    for put in puts:
        put.wait()


def per_device(tiles, tile_rows, tile_cols, tile_count, seeds, decay):
    slots = tiles.shape[0]
    seed_count = seeds.shape[0]
    blk = seeds.shape[1] // TILE
    panels = lax.axis_size("row")
    bufs = panels * NEED
    smem = pl.BlockSpec(memory_space=pltpu.SMEM)
    vmem = pl.BlockSpec(memory_space=pltpu.VMEM)
    hbm = pl.BlockSpec(memory_space=pltpu.HBM)
    dma = pltpu.SemaphoreType.DMA
    mib = 1024 * 1024
    packed = jax.ShapeDtypeStruct((bufs, seed_count, TILE), jnp.bfloat16)
    blocks_shape = (blk, seed_count, TILE)
    blocks = pltpu.VMEM(blocks_shape, jnp.bfloat16)
    acc = pltpu.VMEM((blk + 1, seed_count, TILE), jnp.float32)
    seeds_v = pltpu.VMEM(seeds.shape, seeds.dtype)
    small = pltpu.CompilerParams(vmem_limit_bytes=6 * mib)

    f32, i32 = jnp.float32, jnp.int32
    shape = jax.ShapeDtypeStruct
    group = panels // 2
    halves = [[h * group + g for g in range(group)] for h in range(2)]
    own = lax.axis_index("row").astype(i32).reshape(1)

    def away(x, r):
        return lax.ppermute(x, "row", [(p, p ^ r) for p in range(panels)])

    wanted, near_place, place, row, column, rounded = pl.pallas_call(
        index_kernel,
        out_shape=(shape((group, 1, 2 * NEED), i32), shape((1, slots), i32), shape((1, slots), i32), shape((1, slots), i32),
                   shape((seed_count, 1), f32), shape(blocks_shape, jnp.bfloat16)),
        in_specs=[smem, smem, hbm, hbm, hbm, hbm], out_specs=(vmem,) * 6,
        scratch_shapes=[pltpu.VMEM((1, slots), i32), pltpu.VMEM((1, slots), i32), pltpu.VMEM((1, seed_count), f32),
                        seeds_v, dma((4,))],
        compiler_params=small, name="index",
    )(tile_count, own, in_hbm(tile_cols.reshape(1, slots)), in_hbm(tile_rows.reshape(1, slots)),
      in_hbm(decay.reshape(1, seed_count)), in_hbm(seeds))
    other = away(rounded, group)
    asked = lax.all_to_all(wanted, "row", split_axis=0, concat_axis=0, tiled=True, axis_index_groups=halves)
    asked = asked.reshape(group, 2 * NEED)
    chip = shape((2 * NEED, seed_count, TILE), jnp.bfloat16)
    pair = shape((4 * NEED, seed_count, TILE), jnp.bfloat16)
    chips = group // 2
    sent = pl.pallas_call(
        first_pack_kernel, out_shape=(chip, chip) + (pair,) * (chips - 1),
        in_specs=[smem, smem, vmem, vmem], out_specs=(vmem,) * (chips + 1),
        compiler_params=small, name="first_pack",
    )(own, asked, rounded, other)
    tiles, *sent = lax.optimization_barrier((tiles, *sent))
    turned = pl.pallas_call(
        turn_kernel, out_shape=shape(tiles.shape, tiles.dtype), in_specs=[hbm], out_specs=vmem,
        scratch_shapes=[pltpu.VMEM(tiles.shape, tiles.dtype), dma((8,))],
        compiler_params=pltpu.CompilerParams(vmem_limit_bytes=12 * mib), name="turn_tiles",
        cost_estimate=pl.CostEstimate(flops=6_000_000_000, bytes_accessed=8 * mib, transcendentals=0),
    )(in_hbm(tiles))
    direct = []
    for r in ORDER:
        direct.append(away(sent[r // 2 + 1], r))
    far = away(asked, group)
    arrived = {0: sent[0], 1: away(sent[1], 1)}
    for r, x in zip(ORDER, direct):
        arrived[r] = x
        arrived[r + 1] = away(x, 1)
    outgoing = pl.pallas_call(
        first_step_kernel, out_shape=packed, in_specs=[smem] * 5 + [vmem] * (group + 3), out_specs=vmem,
        scratch_shapes=[pltpu.VMEM(packed.shape, packed.dtype), acc, blocks], compiler_params=small, name="first_step",
    )(near_place, row, own, asked, far, *[arrived[r] for r in range(group)], column, seeds, turned)
    for step in range(1, ITERS):
        arrived = lax.all_to_all(outgoing, "row", split_axis=0, concat_axis=0, tiled=True)
        if step < ITERS - 1:
            outgoing = pl.pallas_call(
                step_kernel, out_shape=packed, in_specs=[smem] * 5 + [vmem] * 4, out_specs=vmem,
                scratch_shapes=[acc, blocks], compiler_params=small, name="step",
            )(place, row, own, asked, far, arrived, column, seeds, turned)
        else:
            iterate, squares = pl.pallas_call(
                last_kernel, out_shape=(shape(seeds.shape, f32), shape((panels, 1, seed_count), f32)),
                in_specs=[smem, smem, vmem, vmem, vmem, vmem], out_specs=(vmem, vmem),
                scratch_shapes=[acc], compiler_params=small, name="last",
            )(place, row, arrived, column, seeds, turned)
    squares = lax.all_to_all(squares, "row", split_axis=0, concat_axis=0, tiled=True)
    return pl.pallas_call(
        scale_kernel, out_shape=shape(seeds.shape, f32), in_specs=[vmem, vmem], out_specs=hbm,
        scratch_shapes=[seeds_v, dma((4,))], compiler_params=small, name="scale")(squares, iterate)


def solution(mesh):
    in_specs = (
        P(("graph", "row"), None, None),
        P(("graph", "row")),
        P(("graph", "row")),
        P(("graph", "row")),
        P(None, ("graph", "row")),
        P(),
    )

    return jax.shard_map(
        per_device, mesh=mesh, in_specs=in_specs, out_specs=P(None, ("graph", "row")), check_vma=False)
```

```python
import jax
import jax.numpy as jnp
from jax import lax
from jax.experimental import pallas as pl
from jax.experimental.pallas import tpu as pltpu
from jax.sharding import PartitionSpec as P


TILE = 256
NEED = 4
ITERS = 3
TURN = 4
ORDER = (4, 5, 2, 3, 6, 7, 1)


def in_hbm(x):
    return pltpu.with_memory_space_constraint(x, pltpu.HBM)


def index_kernel(count_ref, own_ref, cols_ref, rows_ref, decay_ref, seeds_ref, wanted_ref, near_place_ref, place_ref, row_ref, column_ref,
                 rounded_ref, cols_v, rows_v, decay_v, seeds_v, sems):
    blk = rounded_ref.shape[0]
    group = wanted_ref.shape[0]
    panels = 2 * group
    slots = cols_v.shape[1]
    seed_count = seeds_v.shape[0]
    gets = []
    for i, (src, dst) in enumerate(((cols_ref, cols_v), (rows_ref, rows_v), (decay_ref, decay_v), (seeds_ref, seeds_v))):
        gets.append(pltpu.make_async_copy(src, dst, sems.at[i]))
        gets[-1].start()
    gets[0].wait()
    live = lax.broadcasted_iota(jnp.int32, (panels, slots), 1) < count_ref[0]
    panel = lax.broadcasted_iota(jnp.int32, (panels, slots), 0)
    local = jnp.where(live, cols_v[...] - blk * panel, -1)
    rank = jnp.zeros((panels, 1), jnp.float32)
    picks = [jnp.zeros((panels, 1), jnp.float32) for _ in range(NEED)]
    spot = jnp.zeros((panels, slots), jnp.float32)
    first = (NEED * panel).astype(jnp.float32)
    for b in range(blk):
        hit = local == b
        spot = jnp.where(hit, first + rank, spot)
        here = jnp.max(jnp.where(hit, 1.0, 0.0), axis=1, keepdims=True)
        for k in range(NEED):
            picks[k] = jnp.where((here > 0) & (rank == k), float(b), picks[k])
        rank = rank + here
    half = own_ref[0] // group
    own = own_ref[0] % group
    lane = lax.broadcasted_iota(jnp.int32, (group, 2 * NEED), 1)
    wanted = jnp.zeros((group, 2 * NEED), jnp.float32)
    for k in range(NEED):
        near = jnp.where(half == 0, picks[k][:group], picks[k][group:])
        far = jnp.where(half == 0, picks[k][group:], picks[k][:group])
        wanted = jnp.where(lane == k, near, jnp.where(lane == NEED + k, far, wanted))
    wanted = wanted.astype(jnp.int32)
    for g in range(group):
        wanted_ref[g] = wanted[g:g + 1]
    place_ref[...] = jnp.sum(spot, axis=0, keepdims=True).astype(jnp.int32)
    side = jnp.where((panel >= group) == (half == 1), 0, NEED)
    away = (panel % group) ^ own
    shift = (away * 2 * NEED + side - panel * NEED).astype(jnp.float32)
    near_spot = jnp.where(local >= 0, jnp.where(local < blk, spot + shift, 0.0), 0.0)
    near_place_ref[...] = jnp.sum(near_spot, axis=0, keepdims=True).astype(jnp.int32)
    gets[1].wait()
    row_ref[...] = jnp.where(live[:1], rows_v[...], blk)
    gets[2].wait()
    column_ref[...] = to_column(decay_v[...], seed_count)
    gets[3].wait()
    for b in range(blk):
        rounded_ref[b] = seeds_v[:, b * TILE:(b + 1) * TILE].astype(jnp.bfloat16)


def to_column(x, size):
    square = (size, size)
    diagonal = lax.broadcasted_iota(jnp.int32, square, 0) == lax.broadcasted_iota(jnp.int32, square, 1)
    return jnp.sum(jnp.where(diagonal, jnp.broadcast_to(x, square), 0.0), axis=1, keepdims=True)


def first_pack_kernel(own_ref, asked_ref, rounded_ref, other_ref, *out_refs):
    for r, out_ref in enumerate(out_refs):
        g = (own_ref[0] % len(out_refs)) ^ r
        for k in range(NEED):
            out_ref[k] = rounded_ref[asked_ref[g, k]]
            out_ref[NEED + k] = other_ref[asked_ref[g, NEED + k]]


def turn_kernel(tiles_ref, out_ref, buf, sems):
    chunk = buf.shape[0] // sems.shape[0]
    parts = [pl.ds(c * chunk, chunk) for c in range(sems.shape[0])]
    gets = [pltpu.make_async_copy(tiles_ref.at[p], buf.at[p], sems.at[c]) for c, p in enumerate(parts)]
    for get in gets:
        get.start()
    for c, get in enumerate(gets):
        get.wait()

        def body(i, carry, c=c):
            for k in range(TURN):
                t = c * chunk + i * TURN + k
                out_ref[t] = buf[t].T
            return carry

        lax.fori_loop(0, chunk // TURN, body, 0)


def send_blocks(blocks, own_ref, asked_ref, far_ref, out_ref):
    group = asked_ref.shape[0]
    near = own_ref[0] // group * group
    for g in range(group):
        for k in range(NEED):
            out_ref[(near + g) * NEED + k] = blocks[asked_ref[g, k]]
            out_ref[(group - near + g) * NEED + k] = blocks[far_ref[g, NEED + k]]


def products(place_ref, row_ref, arrived_ref, tiles_ref, acc):
    acc[...] = jnp.zeros(acc.shape, acc.dtype)
    for t in range(tiles_ref.shape[0]):
        x = arrived_ref[place_ref[0, t]]
        acc[row_ref[0, t]] += jnp.dot(x, tiles_ref[t], preferred_element_type=jnp.float32)


def update(own_ref, asked_ref, far_ref, decay_ref, seeds_ref, out_ref, acc, blocks):
    decay = decay_ref[...]
    for b in range(blocks.shape[0]):
        blocks[b] = (decay * acc[b] + seeds_ref[:, b * TILE:(b + 1) * TILE]).astype(jnp.bfloat16)
    send_blocks(blocks, own_ref, asked_ref, far_ref, out_ref)


def first_step_kernel(place_ref, row_ref, own_ref, asked_ref, far_ref, *refs):
    arrived_refs, (decay_ref, seeds_ref, tiles_ref, out_ref, arrived, acc, blocks) = refs[:-7], refs[-7:]
    each = 2 * NEED
    for r, ref in enumerate(arrived_refs):
        arrived[r * each:(r + 1) * each] = ref[...]
    products(place_ref, row_ref, arrived, tiles_ref, acc)
    update(own_ref, asked_ref, far_ref, decay_ref, seeds_ref, out_ref, acc, blocks)


def step_kernel(place_ref, row_ref, own_ref, asked_ref, far_ref, arrived_ref, decay_ref, seeds_ref, tiles_ref,
                out_ref, acc, blocks):
    products(place_ref, row_ref, arrived_ref, tiles_ref, acc)
    update(own_ref, asked_ref, far_ref, decay_ref, seeds_ref, out_ref, acc, blocks)


def last_kernel(place_ref, row_ref, arrived_ref, decay_ref, seeds_ref, tiles_ref, out_ref, squares_ref, acc):
    products(place_ref, row_ref, arrived_ref, tiles_ref, acc)
    decay = decay_ref[...]
    total = jnp.zeros((acc.shape[1], 128), jnp.float32)
    for b in range(seeds_ref.shape[1] // TILE):
        x = decay * acc[b] + seeds_ref[:, b * TILE:(b + 1) * TILE]
        out_ref[:, b * TILE:(b + 1) * TILE] = x
        sq = x * x
        total = total + sq[:, :128] + sq[:, 128:]
    squares_ref[...] = jnp.broadcast_to(jnp.sum(total.T, axis=0, keepdims=True)[None], squares_ref.shape)


def scale_kernel(squares_ref, iterate_ref, out_ref, buf, sems):
    seed_count, nodes = iterate_ref.shape
    panels = squares_ref.shape[0]
    total = squares_ref[0]
    for p in range(1, panels):
        total = total + squares_ref[p]
    factor = to_column(1.0 / jnp.sqrt(total / (panels * nodes) + 1e-06), seed_count)
    puts = []
    parts = sems.shape[0]
    for c in range(parts):
        part = pl.ds(c * nodes // parts, nodes // parts)
        buf[:, part] = iterate_ref[:, part] * factor
        puts.append(pltpu.make_async_copy(buf.at[:, part], out_ref.at[:, part], sems.at[c]))
        puts[-1].start()
    for put in puts:
        put.wait()


def per_device(tiles, tile_rows, tile_cols, tile_count, seeds, decay):
    slots = tiles.shape[0]
    seed_count = seeds.shape[0]
    blk = seeds.shape[1] // TILE
    panels = lax.axis_size("row")
    bufs = panels * NEED
    smem = pl.BlockSpec(memory_space=pltpu.SMEM)
    vmem = pl.BlockSpec(memory_space=pltpu.VMEM)
    hbm = pl.BlockSpec(memory_space=pltpu.HBM)
    dma = pltpu.SemaphoreType.DMA
    mib = 1024 * 1024
    packed = jax.ShapeDtypeStruct((bufs, seed_count, TILE), jnp.bfloat16)
    blocks_shape = (blk, seed_count, TILE)
    blocks = pltpu.VMEM(blocks_shape, jnp.bfloat16)
    acc = pltpu.VMEM((blk + 1, seed_count, TILE), jnp.float32)
    seeds_v = pltpu.VMEM(seeds.shape, seeds.dtype)
    small = pltpu.CompilerParams(vmem_limit_bytes=6 * mib)

    f32, i32 = jnp.float32, jnp.int32
    shape = jax.ShapeDtypeStruct
    group = panels // 2
    halves = [[h * group + g for g in range(group)] for h in range(2)]
    own = lax.axis_index("row").astype(i32).reshape(1)

    def away(x, r):
        return lax.ppermute(x, "row", [(p, p ^ r) for p in range(panels)])

    wanted, near_place, place, row, column, rounded = pl.pallas_call(
        index_kernel,
        out_shape=(shape((group, 1, 2 * NEED), i32), shape((1, slots), i32), shape((1, slots), i32), shape((1, slots), i32),
                   shape((seed_count, 1), f32), shape(blocks_shape, jnp.bfloat16)),
        in_specs=[smem, smem, hbm, hbm, hbm, hbm], out_specs=(vmem,) * 6,
        scratch_shapes=[pltpu.VMEM((1, slots), i32), pltpu.VMEM((1, slots), i32), pltpu.VMEM((1, seed_count), f32),
                        seeds_v, dma((4,))],
        compiler_params=small, name="index",
    )(tile_count, own, in_hbm(tile_cols.reshape(1, slots)), in_hbm(tile_rows.reshape(1, slots)),
      in_hbm(decay.reshape(1, seed_count)), in_hbm(seeds))
    other = away(rounded, group)
    asked = lax.all_to_all(wanted, "row", split_axis=0, concat_axis=0, tiled=True, axis_index_groups=halves)
    asked = asked.reshape(group, 2 * NEED)
    sent = pl.pallas_call(
        first_pack_kernel, out_shape=(shape((2 * NEED, seed_count, TILE), jnp.bfloat16),) * group,
        in_specs=[smem, smem, vmem, vmem], out_specs=(vmem,) * group,
        compiler_params=small, name="first_pack",
    )(own, asked, rounded, other)
    tiles, *sent = lax.optimization_barrier((tiles, *sent))
    turned = pl.pallas_call(
        turn_kernel, out_shape=shape(tiles.shape, tiles.dtype), in_specs=[hbm], out_specs=vmem,
        scratch_shapes=[pltpu.VMEM(tiles.shape, tiles.dtype), dma((8,))],
        compiler_params=pltpu.CompilerParams(vmem_limit_bytes=12 * mib), name="turn_tiles",
        cost_estimate=pl.CostEstimate(flops=6_000_000_000, bytes_accessed=8 * mib, transcendentals=0),
    )(in_hbm(tiles))
    arrived = {0: sent[0]}
    for r in ORDER:
        arrived[r] = away(sent[r], r)
    far = away(asked, group)
    outgoing = pl.pallas_call(
        first_step_kernel, out_shape=packed, in_specs=[smem] * 5 + [vmem] * (group + 3), out_specs=vmem,
        scratch_shapes=[pltpu.VMEM(packed.shape, packed.dtype), acc, blocks], compiler_params=small, name="first_step",
    )(near_place, row, own, asked, far, *[arrived[r] for r in range(group)], column, seeds, turned)
    for step in range(1, ITERS):
        arrived = lax.all_to_all(outgoing, "row", split_axis=0, concat_axis=0, tiled=True)
        if step < ITERS - 1:
            outgoing = pl.pallas_call(
                step_kernel, out_shape=packed, in_specs=[smem] * 5 + [vmem] * 4, out_specs=vmem,
                scratch_shapes=[acc, blocks], compiler_params=small, name="step",
            )(place, row, own, asked, far, arrived, column, seeds, turned)
        else:
            iterate, squares = pl.pallas_call(
                last_kernel, out_shape=(shape(seeds.shape, f32), shape((panels, 1, seed_count), f32)),
                in_specs=[smem, smem, vmem, vmem, vmem, vmem], out_specs=(vmem, vmem),
                scratch_shapes=[acc], compiler_params=small, name="last",
            )(place, row, arrived, column, seeds, turned)
    squares = lax.all_to_all(squares, "row", split_axis=0, concat_axis=0, tiled=True)
    return pl.pallas_call(
        scale_kernel, out_shape=shape(seeds.shape, f32), in_specs=[vmem, vmem], out_specs=hbm,
        scratch_shapes=[seeds_v, dma((4,))], compiler_params=small, name="scale")(squares, iterate)


def solution(mesh):
    in_specs = (
        P(("graph", "row"), None, None),
        P(("graph", "row")),
        P(("graph", "row")),
        P(("graph", "row")),
        P(None, ("graph", "row")),
        P(),
    )

    return jax.shard_map(
        per_device, mesh=mesh, in_specs=in_specs, out_specs=P(None, ("graph", "row")), check_vma=False)
```

```python
import jax
import jax.numpy as jnp
from jax import lax
from jax.experimental import pallas as pl
from jax.experimental.pallas import tpu as pltpu
from jax.sharding import PartitionSpec as P


TILE = 256
NEED = 4
ITERS = 3
TURN = 4
FAR = 4
ORDER = (4, 5, 2, 3, 6, 7, 1)


def in_hbm(x):
    return pltpu.with_memory_space_constraint(x, pltpu.HBM)


def index_kernel(count_ref, own_ref, cols_ref, rows_ref, decay_ref, seeds_ref, wanted_ref, near_place_ref, place_ref, row_ref, column_ref,
                 rounded_ref, cols_v, rows_v, decay_v, seeds_v, sems):
    blk = rounded_ref.shape[0]
    group = wanted_ref.shape[0]
    panels = 2 * group
    slots = cols_v.shape[1]
    seed_count = seeds_v.shape[0]
    gets = []
    for i, (src, dst) in enumerate(((cols_ref, cols_v), (rows_ref, rows_v), (decay_ref, decay_v), (seeds_ref, seeds_v))):
        gets.append(pltpu.make_async_copy(src, dst, sems.at[i]))
        gets[-1].start()
    gets[0].wait()
    live = lax.broadcasted_iota(jnp.int32, (panels, slots), 1) < count_ref[0]
    panel = lax.broadcasted_iota(jnp.int32, (panels, slots), 0)
    local = jnp.where(live, cols_v[...] - blk * panel, -1)
    rank = jnp.zeros((panels, 1), jnp.float32)
    picks = [jnp.zeros((panels, 1), jnp.float32) for _ in range(NEED)]
    spot = jnp.zeros((panels, slots), jnp.float32)
    first = (NEED * panel).astype(jnp.float32)
    for b in range(blk):
        hit = local == b
        spot = jnp.where(hit, first + rank, spot)
        here = jnp.max(jnp.where(hit, 1.0, 0.0), axis=1, keepdims=True)
        for k in range(NEED):
            picks[k] = jnp.where((here > 0) & (rank == k), float(b), picks[k])
        rank = rank + here
    half = own_ref[0] // group
    own = own_ref[0] % group
    lane = lax.broadcasted_iota(jnp.int32, (group, 2 * NEED), 1)
    wanted = jnp.zeros((group, 2 * NEED), jnp.float32)
    for k in range(NEED):
        near = jnp.where(half == 0, picks[k][:group], picks[k][group:])
        far = jnp.where(half == 0, picks[k][group:], picks[k][:group])
        wanted = jnp.where(lane == k, near, jnp.where(lane == NEED + k, far, wanted))
    wanted = wanted.astype(jnp.int32)
    for g in range(group):
        wanted_ref[g] = wanted[g:g + 1]
    place_ref[...] = jnp.sum(spot, axis=0, keepdims=True).astype(jnp.int32)
    side = jnp.where((panel >= group) == (half == 1), 0, NEED)
    away = (panel % group) ^ own
    shift = (away * 2 * NEED + side - panel * NEED).astype(jnp.float32)
    whole = (away >= FAR) & (away < FAR + 2) & (side == 0)
    behind = (panels * NEED + (away - FAR) * blk + local).astype(jnp.float32)
    near_spot = jnp.where((local >= 0) & (local < blk), jnp.where(whole, behind, spot + shift), 0.0)
    near_place_ref[...] = jnp.sum(near_spot, axis=0, keepdims=True).astype(jnp.int32)
    gets[1].wait()
    row_ref[...] = jnp.where(live[:1], rows_v[...], blk)
    gets[2].wait()
    column_ref[...] = to_column(decay_v[...], seed_count)
    gets[3].wait()
    for b in range(blk):
        rounded_ref[b] = seeds_v[:, b * TILE:(b + 1) * TILE].astype(jnp.bfloat16)


def to_column(x, size):
    square = (size, size)
    diagonal = lax.broadcasted_iota(jnp.int32, square, 0) == lax.broadcasted_iota(jnp.int32, square, 1)
    return jnp.sum(jnp.where(diagonal, jnp.broadcast_to(x, square), 0.0), axis=1, keepdims=True)


def first_pack_kernel(own_ref, asked_ref, rounded_ref, other_ref, *out_refs):
    for r, out_ref in enumerate(out_refs):
        g = (own_ref[0] % len(out_refs)) ^ r
        skip = out_ref.shape[0] - NEED
        for k in range(NEED):
            if skip:
                out_ref[k] = rounded_ref[asked_ref[g, k]]
            out_ref[skip + k] = other_ref[asked_ref[g, NEED + k]]


def turn_kernel(tiles_ref, out_ref):
    def body(i, carry):
        for k in range(TURN):
            out_ref[i * TURN + k] = tiles_ref[i * TURN + k].T
        return carry

    lax.fori_loop(0, tiles_ref.shape[0] // TURN, body, 0)


def send_blocks(blocks, own_ref, asked_ref, far_ref, out_ref):
    group = asked_ref.shape[0]
    near = own_ref[0] // group * group
    for g in range(group):
        for k in range(NEED):
            out_ref[(near + g) * NEED + k] = blocks[asked_ref[g, k]]
            out_ref[(group - near + g) * NEED + k] = blocks[far_ref[g, NEED + k]]


def products(place_ref, row_ref, arrived_ref, tiles_ref, acc):
    acc[...] = jnp.zeros(acc.shape, acc.dtype)
    for t in range(tiles_ref.shape[0]):
        x = arrived_ref[place_ref[0, t]]
        acc[row_ref[0, t]] += jnp.dot(x, tiles_ref[t], preferred_element_type=jnp.float32)


def update(own_ref, asked_ref, far_ref, decay_ref, seeds_ref, out_ref, acc, blocks):
    decay = decay_ref[...]
    for b in range(blocks.shape[0]):
        blocks[b] = (decay * acc[b] + seeds_ref[:, b * TILE:(b + 1) * TILE]).astype(jnp.bfloat16)
    send_blocks(blocks, own_ref, asked_ref, far_ref, out_ref)


def first_step_kernel(place_ref, row_ref, own_ref, asked_ref, far_ref, *refs):
    arrived_refs, (decay_ref, seeds_ref, tiles_ref, out_ref, arrived, acc, blocks) = refs[:-7], refs[-7:]
    each = 2 * NEED
    at = 0
    for ref in arrived_refs:
        count = ref.shape[0]
        at += each - count if count < each else 0
        arrived[at:at + count] = ref[...]
        at += count
    products(place_ref, row_ref, arrived, tiles_ref, acc)
    update(own_ref, asked_ref, far_ref, decay_ref, seeds_ref, out_ref, acc, blocks)


def step_kernel(place_ref, row_ref, own_ref, asked_ref, far_ref, arrived_ref, decay_ref, seeds_ref, tiles_ref,
                out_ref, acc, blocks):
    products(place_ref, row_ref, arrived_ref, tiles_ref, acc)
    update(own_ref, asked_ref, far_ref, decay_ref, seeds_ref, out_ref, acc, blocks)


def last_kernel(place_ref, row_ref, arrived_ref, decay_ref, seeds_ref, tiles_ref, out_ref, squares_ref, acc):
    products(place_ref, row_ref, arrived_ref, tiles_ref, acc)
    decay = decay_ref[...]
    total = jnp.zeros((acc.shape[1], 128), jnp.float32)
    for b in range(seeds_ref.shape[1] // TILE):
        x = decay * acc[b] + seeds_ref[:, b * TILE:(b + 1) * TILE]
        out_ref[:, b * TILE:(b + 1) * TILE] = x
        sq = x * x
        total = total + sq[:, :128] + sq[:, 128:]
    squares_ref[...] = jnp.broadcast_to(jnp.sum(total.T, axis=0, keepdims=True)[None], squares_ref.shape)


def scale_kernel(squares_ref, iterate_ref, out_ref, buf, sems):
    seed_count, nodes = iterate_ref.shape
    panels = squares_ref.shape[0]
    total = squares_ref[0]
    for p in range(1, panels):
        total = total + squares_ref[p]
    factor = to_column(1.0 / jnp.sqrt(total / (panels * nodes) + 1e-06), seed_count)
    puts = []
    parts = sems.shape[0]
    for c in range(parts):
        part = pl.ds(c * nodes // parts, nodes // parts)
        buf[:, part] = iterate_ref[:, part] * factor
        puts.append(pltpu.make_async_copy(buf.at[:, part], out_ref.at[:, part], sems.at[c]))
        puts[-1].start()
    for put in puts:
        put.wait()


def per_device(tiles, tile_rows, tile_cols, tile_count, seeds, decay):
    slots = tiles.shape[0]
    seed_count = seeds.shape[0]
    blk = seeds.shape[1] // TILE
    panels = lax.axis_size("row")
    bufs = panels * NEED
    smem = pl.BlockSpec(memory_space=pltpu.SMEM)
    vmem = pl.BlockSpec(memory_space=pltpu.VMEM)
    hbm = pl.BlockSpec(memory_space=pltpu.HBM)
    dma = pltpu.SemaphoreType.DMA
    mib = 1024 * 1024
    packed = jax.ShapeDtypeStruct((bufs, seed_count, TILE), jnp.bfloat16)
    blocks_shape = (blk, seed_count, TILE)
    blocks = pltpu.VMEM(blocks_shape, jnp.bfloat16)
    acc = pltpu.VMEM((blk + 1, seed_count, TILE), jnp.float32)
    seeds_v = pltpu.VMEM(seeds.shape, seeds.dtype)
    small = pltpu.CompilerParams(vmem_limit_bytes=6 * mib)

    f32, i32 = jnp.float32, jnp.int32
    shape = jax.ShapeDtypeStruct
    group = panels // 2
    halves = [[h * group + g for g in range(group)] for h in range(2)]
    own = lax.axis_index("row").astype(i32).reshape(1)

    def away(x, r):
        return lax.ppermute(x, "row", [(p, p ^ r) for p in range(panels)])

    wanted, near_place, place, row, column, rounded = pl.pallas_call(
        index_kernel,
        out_shape=(shape((group, 1, 2 * NEED), i32), shape((1, slots), i32), shape((1, slots), i32), shape((1, slots), i32),
                   shape((seed_count, 1), f32), shape(blocks_shape, jnp.bfloat16)),
        in_specs=[smem, smem, hbm, hbm, hbm, hbm], out_specs=(vmem,) * 6,
        scratch_shapes=[pltpu.VMEM((1, slots), i32), pltpu.VMEM((1, slots), i32), pltpu.VMEM((1, seed_count), f32),
                        seeds_v, dma((4,))],
        compiler_params=small, name="index",
    )(tile_count, own, in_hbm(tile_cols.reshape(1, slots)), in_hbm(tile_rows.reshape(1, slots)),
      in_hbm(decay.reshape(1, seed_count)), in_hbm(seeds))
    other = away(rounded, group)
    cross = away(rounded, FAR)
    asked = lax.all_to_all(wanted, "row", split_axis=0, concat_axis=0, tiled=True, axis_index_groups=halves)
    asked = asked.reshape(group, 2 * NEED)
    sent = pl.pallas_call(
        first_pack_kernel, out_shape=tuple(shape(((1 if r // 2 * 2 == FAR else 2) * NEED, seed_count, TILE), jnp.bfloat16)
                                           for r in range(group)),
        in_specs=[smem, smem, vmem, vmem], out_specs=(vmem,) * group,
        compiler_params=small, name="first_pack",
        cost_estimate=pl.CostEstimate(flops=20_000_000_000, bytes_accessed=2 * mib, transcendentals=0),
    )(own, asked, rounded, other)
    tiles, *sent = lax.optimization_barrier((tiles, *sent))
    turned = pl.pallas_call(
        turn_kernel, out_shape=shape(tiles.shape, tiles.dtype), in_specs=[vmem], out_specs=vmem,
        compiler_params=small, name="turn_tiles",
        cost_estimate=pl.CostEstimate(flops=6_000_000_000, bytes_accessed=8 * mib, transcendentals=0),
    )(tiles)
    arrived = {0: sent[0]}
    for r in ORDER:
        arrived[r] = away(sent[r], r)
    far = away(asked, group)
    crossed = away(cross, 1)
    outgoing = pl.pallas_call(
        first_step_kernel, out_shape=packed, in_specs=[smem] * 5 + [vmem] * (group + 5), out_specs=vmem,
        scratch_shapes=[pltpu.VMEM((bufs + 2 * blk, seed_count, TILE), packed.dtype), acc, blocks], compiler_params=small, name="first_step",
    )(near_place, row, own, asked, far, *[arrived[r] for r in range(group)], cross, crossed, column, seeds, turned)
    for step in range(1, ITERS):
        arrived = lax.all_to_all(outgoing, "row", split_axis=0, concat_axis=0, tiled=True)
        if step < ITERS - 1:
            outgoing = pl.pallas_call(
                step_kernel, out_shape=packed, in_specs=[smem] * 5 + [vmem] * 4, out_specs=vmem,
                scratch_shapes=[acc, blocks], compiler_params=small, name="step",
            )(place, row, own, asked, far, arrived, column, seeds, turned)
        else:
            iterate, squares = pl.pallas_call(
                last_kernel, out_shape=(shape(seeds.shape, f32), shape((panels, 1, seed_count), f32)),
                in_specs=[smem, smem, vmem, vmem, vmem, vmem], out_specs=(vmem, vmem),
                scratch_shapes=[acc], compiler_params=small, name="last",
            )(place, row, arrived, column, seeds, turned)
    squares = lax.all_to_all(squares, "row", split_axis=0, concat_axis=0, tiled=True)
    return pl.pallas_call(
        scale_kernel, out_shape=shape(seeds.shape, f32), in_specs=[vmem, vmem], out_specs=hbm,
        scratch_shapes=[seeds_v, dma((4,))], compiler_params=small, name="scale")(squares, iterate)


def solution(mesh):
    in_specs = (
        P(("graph", "row"), None, None),
        P(("graph", "row")),
        P(("graph", "row")),
        P(("graph", "row")),
        P(None, ("graph", "row")),
        P(),
    )

    return jax.shard_map(
        per_device, mesh=mesh, in_specs=in_specs, out_specs=P(None, ("graph", "row")), check_vma=False)
```
